256 devices in a mesh: section: 16 (over x, y), tensor: 16 (over z, core).
Axes of the slice: x: 4, y: 4, z: 8, core: 2. Of those that a mesh axis runs over, the one named last changes fastest.
Arguments:
- token_ids: int32 [3, 48], replicated, may hold values from 0 to 31999
- emb_table: bfloat16 [32000, 4096], P('section', 'tensor'), may hold values from -6 to 6
- attn_gain: bfloat16 [16, 4096], P('section'), may hold values from 0.25 to 1.75
- query_weight: bfloat16 [16, 4096, 4096], P('section', None, 'tensor'), may hold values from -8 to 8
- key_weight: bfloat16 [16, 4096, 4096], P('section', None, 'tensor'), may hold values from -8 to 8
- value_weight: bfloat16 [16, 4096, 4096], P('section', None, 'tensor'), may hold values from -0.09375 to 0.09375
- mix_weight: float32 [16, 32], P('section', 'tensor'), may hold values from 0.2 to 0.8
- out_weight: bfloat16 [16, 4096, 4096], P('section', 'tensor'), may hold values from -0.125 to 0.125
Outputs:
- layer_outputs: bfloat16 [16, 3, 48, 4096], P('section', None, None, 'tensor')
The draws below stay inside these ranges and needn't reach their ends.
All inputs are finite; a program needn't handle non-finite values.
Results may differ from the reference program's by a relative error of at most 0.033.
Values may be sent and summed in bfloat16 or wider, within the bound.
No kernel may reach another device: no remote copies, remote signals or barrier semaphores. Data moves between devices by JAX's collectives and lax.ppermute only.
A program may use at most 64 MiB of HBM per device.

```python
import jax
import jax.numpy as jnp
from jax import lax

D = 4096
HEADS = 32
HEAD_DIM = 128
VOCAB = 32000
MICRO = 3
SEQ = 48
LAYERS = 16
N_TENSOR = 16


def weight_pair(key):
    query_key = jax.random.fold_in(key, 101)
    other_key = jax.random.fold_in(key, 202)
    shape = (LAYERS, D, HEADS * HEAD_DIM)
    base_draw = jax.random.normal(query_key, shape, jnp.float32) * D ** (-0.5)
    other_draw = jax.random.normal(other_key, shape, jnp.float32) * D ** (-0.5)
    return (base_draw, other_draw)


def draw_query_weight(key, part):
    return jnp.clip(weight_pair(key)[0], -8.0, 8.0).astype(jnp.bfloat16)


def draw_key_weight(key, part):
    return jnp.clip(weight_pair(key)[1], -8.0, 8.0).astype(jnp.bfloat16)


def plant(drawn, own_key, low, top_value):
    dims = drawn.shape
    spot = [jax.random.randint(jax.random.fold_in(own_key, axis), (), 0, dims[axis]) for axis in range(len(dims))]
    drawn = drawn.at[tuple(spot)].set(low)
    longest = dims.index(max(dims))
    spot[longest] = (spot[longest] + 1) % dims[longest]
    return drawn.at[tuple(spot)].set(top_value)


def strengthened(result, key, source, target, parts, factor):
    def block_of(axis_at):
        return (jnp.arange(result.shape[axis_at]) // (result.shape[axis_at] // parts)).reshape((-1,) + (1,) * (result.ndim - 1 - axis_at))

    near = jax.random.permutation(key, parts)[block_of(target)]
    other_side = (block_of(target) + parts // 2) % parts
    return jnp.where((block_of(source) == near) | (block_of(source) == other_side), factor * result, result)


def block_levels(key, dims, pieces, least, top_value):
    loudness = 1.0
    for axis_at, parts in pieces:
        heights = jax.random.uniform(jax.random.fold_in(jax.random.fold_in(key, 6), axis_at), (parts,), jnp.float32, least / len(pieces), top_value / len(pieces))
        loudness = loudness * jnp.repeat(jnp.exp(heights), dims[axis_at] // parts).reshape((-1,) + (1,) * (len(dims) - 1 - axis_at))
    return loudness


def normal_values(rng, extent, scale, limit, cuts=(), held_as=jnp.bfloat16):
    drawn = jax.random.normal(rng, extent, jnp.float32) * scale
    if len(cuts) > 0:
        drawn = block_levels(rng, extent, cuts, -0.22, 0.18) * drawn
    return jnp.clip(drawn, min=-limit, max=limit).astype(held_as)


def heavy_noise(key, extent, width, bound, cuts, heavy, kind=jnp.bfloat16):
    array = width * jax.random.normal(key, extent, jnp.float32)
    if cuts:
        array = array * block_levels(key, extent, cuts, -0.22, 0.18)
    return jnp.clip(strengthened(array, jax.random.fold_in(key, 3), *heavy), -bound, bound).astype(kind)


def setup_inputs(seed: int = 0) -> dict:
    streams_of = jax.random.split(jax.random.key(seed), 9)
    token_ids = plant(jax.random.randint(streams_of[0], (MICRO, SEQ), 0, VOCAB), jax.random.fold_in(streams_of[0], 1), 0, VOCAB - 1).astype(jnp.int32)
    emb_table = normal_values(streams_of[1], (VOCAB, D), 1.0, 6.0, ((0, 16), (1, 16)))
    attn_gain = jnp.clip(1.0 + 0.15 * jax.random.normal(streams_of[2], (LAYERS, D), jnp.float32), 0.25, 1.75).astype(jnp.bfloat16)
    query_weight = draw_query_weight(jax.random.fold_in(streams_of[8], 71), 0)
    key_weight = draw_key_weight(jax.random.fold_in(streams_of[8], 71), 0)
    value_weight = normal_values(streams_of[5], (LAYERS, D, HEADS * HEAD_DIM), D ** -0.5, 0.09375, ((0, 16), (2, 16)))
    mix_weight = jnp.clip(0.2 + 0.6 * jax.random.uniform(streams_of[6], (LAYERS, HEADS), jnp.float32) ** block_levels(streams_of[6], (LAYERS, HEADS), ((0, 16), (1, 16)), -0.2, 0.2), 0.2, 0.8)
    out_weight = heavy_noise(streams_of[7], (LAYERS, HEADS * HEAD_DIM, D), (HEADS * HEAD_DIM) ** -0.5, 0.125, ((0, 16), (1, 16)), (1, 2, 16, 2.0))
    return {"token_ids": token_ids, "emb_table": emb_table, "attn_gain": attn_gain, "query_weight": query_weight, "key_weight": key_weight, "value_weight": value_weight, "mix_weight": mix_weight, "out_weight": out_weight}


EPSILON = 1e-05
ROTARY_BASE = 10000.0

def rms_scale(values, norm_gain):
    mean_square = lax.optimization_barrier(jnp.mean(values * values, axis=-1, keepdims=True))
    return values * lax.rsqrt(mean_square + EPSILON) * norm_gain

def rotate(values):
    length = values.shape[-3]
    head_dim = values.shape[-1]
    half_dim = head_dim // 2
    positions = jnp.arange(length, dtype=jnp.float32)
    frequency = ROTARY_BASE ** (-(jnp.arange(half_dim, dtype=jnp.float32) * 2.0) / head_dim)
    angles = positions[:, None] * frequency[None, :]
    cosine = jnp.cos(angles)[:, None, :]
    sine_table = jnp.sin(angles)[:, None, :]
    leading = values[..., :half_dim]
    second = values[..., half_dim:]
    return jnp.concatenate([leading * cosine - second * sine_table, second * cosine + leading * sine_table], axis=-1)

def attend(queries, key_rows, mixed_values):
    length = queries.shape[1]
    scores = jnp.einsum('mqhd,mkhd->mhqk', queries.astype(jnp.float32), key_rows.astype(jnp.float32)) * HEAD_DIM ** (-0.5)
    causal = jnp.arange(length)[:, None] >= jnp.arange(length)[None, :]
    scores = jnp.where(causal, scores, -1e+30)
    row_top = lax.optimization_barrier(jnp.max(scores, axis=-1, keepdims=True))
    expo = jnp.exp(scores - row_top)
    attn_probs = (expo / lax.optimization_barrier(jnp.sum(expo, axis=-1, keepdims=True))).astype(jnp.bfloat16)
    attended = jnp.einsum('mhqk,mkhd->mqhd', attn_probs.astype(jnp.float32), mixed_values.astype(jnp.float32))
    return attended.astype(jnp.bfloat16)

def reference(token_ids, emb_table, attn_gain, query_weight, key_weight, value_weight, mix_weight, out_weight):
    batches, length = token_ids.shape
    first_rows = jnp.take(emb_table, token_ids.reshape(-1).astype(jnp.int32), axis=0)
    first_float = first_rows.astype(jnp.float32)
    first_norm = rms_scale(first_float, attn_gain[0].astype(jnp.float32)).astype(jnp.bfloat16)
    first_values = jnp.dot(first_norm, value_weight[0], preferred_element_type=jnp.float32).astype(jnp.bfloat16)
    source_values = first_values.reshape(batches, length, HEADS, HEAD_DIM).astype(jnp.float32)
    hidden = first_rows.reshape(batches, length, D)
    collected = []
    for layer_index in range(LAYERS):
        norm_gain = attn_gain[layer_index].astype(jnp.float32)
        normed = rms_scale(hidden.astype(jnp.float32), norm_gain).astype(jnp.bfloat16).reshape(-1, D)
        queries = jnp.dot(normed, query_weight[layer_index], preferred_element_type=jnp.float32)
        key_rows = jnp.dot(normed, key_weight[layer_index], preferred_element_type=jnp.float32)
        values = jnp.dot(normed, value_weight[layer_index], preferred_element_type=jnp.float32)
        queries = rotate(queries.reshape(batches, length, HEADS, HEAD_DIM)).astype(jnp.bfloat16)
        key_rows = rotate(key_rows.reshape(batches, length, HEADS, HEAD_DIM)).astype(jnp.bfloat16)
        values = values.reshape(batches, length, HEADS, HEAD_DIM)
        mix_rate = mix_weight[layer_index][:, None]
        mixed_values = (mix_rate * values + (1.0 - mix_rate) * source_values).astype(jnp.bfloat16)
        attended = attend(queries, key_rows, mixed_values).reshape(batches, length, N_TENSOR, -1)
        out_groups = out_weight[layer_index].reshape(N_TENSOR, -1, D)
        partial_value = jnp.einsum('msgc,gcd->gmsd', attended.astype(jnp.float32), out_groups.astype(jnp.float32))
        partial_value = lax.optimization_barrier(partial_value.astype(jnp.bfloat16)).astype(jnp.float32)
        summed = lax.optimization_barrier(jnp.sum(partial_value, axis=0))
        hidden = (hidden.astype(jnp.float32) + summed).astype(jnp.bfloat16)
        collected.append(hidden)
    return jnp.stack(collected)
```

```python
import functools

import jax
import jax.numpy as jnp
from jax import lax
from jax.experimental import pallas as pl
from jax.experimental.pallas import tpu as pltpu
from jax.sharding import PartitionSpec as P

EPSILON = 1e-05
ROTARY_BASE = 10000.0
HEAD_DIM = 128
VMEM = pltpu.VMEM
PIECES = 4


def rotary_tables(length):
    half_dim = HEAD_DIM // 2
    positions = jnp.arange(length, dtype=jnp.float32)
    frequency = ROTARY_BASE ** (-(jnp.arange(half_dim, dtype=jnp.float32) * 2.0) / HEAD_DIM)
    angles = positions[:, None] * frequency[None, :]
    cosine, sine = jnp.cos(angles), jnp.sin(angles)
    return (
        jnp.concatenate([cosine, cosine], axis=-1),
        jnp.concatenate([-sine, sine], axis=-1),
    )


def layer_kernel(
    flags, x_ref, gain_ref, source_ref, mix_ref, cos_ref, sin_ref, wq, wk, wv, wo,
    keep_ref, give_ref, carried_ref, normed, w_in, w_out, sem_in, sem_out,
):
    shards, length, width = x_ref.shape
    depth = shards * width
    rows = depth // PIECES
    core, is_first = flags[0], flags[1]

    def in_copy(piece, which):
        span = pl.ds(piece * rows, rows)
        source = (wq, wk, wv)[which]
        return pltpu.make_async_copy(
            source.at[span, :],
            w_in.at[span, pl.ds(which * width, width)],
            sem_in.at[piece, which],
        )

    out_copy = pltpu.make_async_copy(wo, w_out, sem_out)
    for piece in range(PIECES):
        for which in range(3):
            in_copy(piece, which).start()
    out_copy.start()

    square = jnp.zeros((length, width), jnp.float32)
    for j in range(shards):
        value = x_ref[j].astype(jnp.float32)
        square = square + value * value
    scale = lax.rsqrt(jnp.sum(square, axis=-1, keepdims=True) * (1.0 / depth) + EPSILON)
    for j in range(shards):
        value = x_ref[j].astype(jnp.float32) * scale * gain_ref[j][None, :]
        normed[:, j * width : (j + 1) * width] = value.astype(jnp.bfloat16)

    total = jnp.zeros((length, 3 * width), jnp.float32)
    for piece in range(PIECES):
        for which in range(3):
            in_copy(piece, which).wait()
        total = total + jnp.dot(
            normed[:, piece * rows : (piece + 1) * rows],
            w_in[piece * rows : (piece + 1) * rows, :],
            preferred_element_type=jnp.float32,
        )
    values = total[:, 2 * width :]
    source = jnp.where(is_first == 1, values.astype(jnp.bfloat16), source_ref[...])
    carried_ref[...] = source
    mix = mix_ref[...]
    mixed = (mix * values + (1.0 - mix) * source.astype(jnp.float32)).astype(jnp.bfloat16)
    cosine, sine = cos_ref[...], sin_ref[...]
    causal = lax.broadcasted_iota(jnp.int32, (length, length), 0) >= lax.broadcasted_iota(
        jnp.int32, (length, length), 1
    )

    def rotated(part):
        return (part * cosine + pltpu.roll(part, HEAD_DIM // 2, 1) * sine).astype(jnp.bfloat16)

    attended = []
    for head in range(width // HEAD_DIM):
        low = head * HEAD_DIM
        query = rotated(total[:, low : low + HEAD_DIM])
        key = rotated(total[:, width + low : width + low + HEAD_DIM])
        scores = lax.dot_general(
            query, key, (((1,), (1,)), ((), ())), preferred_element_type=jnp.float32
        ) * HEAD_DIM ** (-0.5)
        scores = jnp.where(causal, scores, -1e30)
        expo = jnp.exp(scores - jnp.max(scores, axis=-1, keepdims=True))
        probs = (expo / jnp.sum(expo, axis=-1, keepdims=True)).astype(jnp.bfloat16)
        attended.append(
            jnp.dot(
                probs, mixed[:, low : low + HEAD_DIM], preferred_element_type=jnp.float32
            ).astype(jnp.bfloat16)
        )
    attended = jnp.concatenate(attended, axis=-1)
    out_copy.wait()
    for chip in range(shards // 2):
        for target, side in ((give_ref, 1 - core), (keep_ref, core)):
            low = pl.multiple_of((2 * chip + side) * width, width)
            target[chip] = jnp.dot(
                attended, w_out[:, pl.ds(low, width)], preferred_element_type=jnp.float32
            ).astype(jnp.bfloat16)


def run_layer(flags, x, gain, source, mix, cosine, sine, wq, wk, wv, wo):
    shards, length, width = x.shape
    depth = shards * width
    full = pl.BlockSpec(memory_space=VMEM)
    anywhere = pl.BlockSpec(memory_space=pl.ANY)
    half = jax.ShapeDtypeStruct((shards // 2, length, width), jnp.bfloat16)
    return pl.pallas_call(
        layer_kernel,
        out_shape=(half, half, jax.ShapeDtypeStruct((length, width), jnp.bfloat16)),
        in_specs=[pl.BlockSpec(memory_space=pltpu.SMEM)] + [full] * 6 + [anywhere] * 4,
        out_specs=(full, full, full),
        scratch_shapes=[
            VMEM((length, depth), jnp.bfloat16),
            VMEM((depth, 3 * width), jnp.bfloat16),
            VMEM((width, depth), jnp.bfloat16),
            pltpu.SemaphoreType.DMA((PIECES, 3)),
            pltpu.SemaphoreType.DMA,
        ],
        compiler_params=pltpu.CompilerParams(vmem_limit_bytes=24 * 1024 * 1024),
        name="layer",
    )(flags, x, gain, source, mix, cosine, sine, wq, wk, wv, wo)


def close_kernel(flags, arrived_ref, rows_ref, first_ref, old_ref, send_ref, outputs_ref):
    is_last, following, micro, is_valid = flags[0], flags[1], flags[2], flags[3]
    summed = rows_ref[...].astype(jnp.float32)
    partial = arrived_ref[0].astype(jnp.float32)
    for j in range(1, arrived_ref.shape[0]):
        partial = partial + arrived_ref[j].astype(jnp.float32)
    fresh = (summed + partial).astype(jnp.bfloat16)
    send_ref[...] = jnp.where(is_last == 1, first_ref[following], fresh)
    for m in range(outputs_ref.shape[0]):
        outputs_ref[m] = jnp.where((micro == m) & (is_valid == 1), fresh, old_ref[m])


def close_layer(flags, arrived, rows, first, outputs):
    full = pl.BlockSpec(memory_space=VMEM)
    return pl.pallas_call(
        close_kernel,
        out_shape=(
            jax.ShapeDtypeStruct(rows.shape, jnp.bfloat16),
            jax.ShapeDtypeStruct(outputs.shape, jnp.bfloat16),
        ),
        in_specs=[pl.BlockSpec(memory_space=pltpu.SMEM)] + [full] * 4,
        out_specs=(full, full),
        compiler_params=pltpu.CompilerParams(vmem_limit_bytes=8 * 1024 * 1024),
        name="close",
    )(flags, arrived, rows, first, outputs)


def shards(
    token_ids, emb_table, attn_gain, query_weight, key_weight, value_weight, mix_weight, out_weight
):
    section_rank = lax.axis_index("section")
    section_count = lax.axis_size("section")
    tensor_rank = lax.axis_index("tensor")
    tensor_count = lax.axis_size("tensor")
    batches, length = token_ids.shape
    vocab_local, width = emb_table.shape
    chips = tensor_count // 2
    same_core = [[2 * chip + core for chip in range(chips)] for core in range(2)]
    gain = attn_gain[0].astype(jnp.float32).reshape(tensor_count, width)
    weights = (query_weight[0], key_weight[0], value_weight[0], out_weight[0])
    mix = jnp.repeat(mix_weight[0], HEAD_DIM)[None, :]
    cosine, sine = rotary_tables(length)
    is_first = (section_rank == 0).astype(jnp.int32)
    is_last = (section_rank == section_count - 1).astype(jnp.int32)
    layer_flags = jnp.stack([lax.rem(tensor_rank, 2), is_first]).astype(jnp.int32)

    flat_ids = token_ids.reshape(-1) - section_rank * vocab_local
    one_hot = (flat_ids[:, None] == jnp.arange(vocab_local, dtype=jnp.int32)[None, :]).astype(
        jnp.bfloat16
    )
    looked = jnp.dot(one_hot, emb_table, preferred_element_type=jnp.float32).astype(jnp.bfloat16)
    found = lax.all_to_all(
        jnp.broadcast_to(looked[None], (section_count, *looked.shape)), "section", 0, 0, tiled=True
    )
    first = found.astype(jnp.float32).sum(axis=0).astype(jnp.bfloat16)
    first = first.reshape(batches, length, width)
    ring = [(s, (s + 1) % section_count) for s in range(section_count)]
    partner = [(t, t ^ 1) for t in range(tensor_count)]

    def advance(step, state):
        rows, source, outputs = state
        position = step - section_rank
        is_valid = ((position >= 0) & (position < batches)).astype(jnp.int32)
        micro = jnp.clip(position, 0, batches - 1)
        following = jnp.minimum(step + 1, batches - 1)
        close_flags = jnp.stack([is_last, following, micro, is_valid]).astype(jnp.int32)
        full = lax.all_gather(rows, "tensor", axis=0, tiled=True)
        full = full.reshape(tensor_count, length, width)
        keep, give, carried = run_layer(
            layer_flags, full, gain, source, mix, cosine, sine, *weights
        )
        given = lax.ppermute(give, "tensor", partner)
        pair = (keep.astype(jnp.float32) + given.astype(jnp.float32)).astype(jnp.bfloat16)
        arrived = lax.all_to_all(pair, "tensor", 0, 0, axis_index_groups=same_core, tiled=True)
        send, outputs = close_layer(close_flags, arrived, rows, first, outputs)
        rows = lax.ppermute(send, "section", ring)
        source = lax.ppermute(carried, "section", ring)
        return rows, source, outputs

    source = jnp.zeros((length, width), jnp.bfloat16)
    outputs = jnp.zeros((batches, length, width), jnp.bfloat16)
    step_count = batches + section_count - 1
    _, _, outputs = lax.fori_loop(0, step_count, advance, (first[0], source, outputs))
    return outputs[None]


def solution(mesh):
    in_specs = (
        P(),
        P("section", "tensor"),
        P("section", None),
        P("section", None, "tensor"),
        P("section", None, "tensor"),
        P("section", None, "tensor"),
        P("section", "tensor"),
        P("section", "tensor", None),
    )
    out_specs = P("section", None, None, "tensor")
    return jax.shard_map(shards, mesh=mesh, in_specs=in_specs, out_specs=out_specs, check_vma=False)
```

```python
import functools

import jax
import jax.numpy as jnp
from jax import lax
from jax.experimental import pallas as pl
from jax.experimental.pallas import tpu as pltpu
from jax.sharding import PartitionSpec as P

EPSILON = 1e-05
ROTARY_BASE = 10000.0
HEAD_DIM = 128
VMEM = pltpu.VMEM
PIECES = 4
SHIFTS = ((4, 1, 7, 0), (3, 5, 2, 6))


def rotary_tables(length):
    half_dim = HEAD_DIM // 2
    positions = jnp.arange(length, dtype=jnp.float32)
    frequency = ROTARY_BASE ** (-(jnp.arange(half_dim, dtype=jnp.float32) * 2.0) / HEAD_DIM)
    angles = positions[:, None] * frequency[None, :]
    cosine, sine = jnp.cos(angles), jnp.sin(angles)
    return (
        jnp.concatenate([cosine, cosine], axis=-1),
        jnp.concatenate([-sine, sine], axis=-1),
    )


def layer_kernel(
    flags, own_ref, other_ref, gain_ref, source_ref, mix_ref, cos_ref, sin_ref, wq, wk, wv, wo,
    keep_ref, give_ref, carried_ref, normed, w_in, w_out, sem_in, sem_out,
):
    chips, length, width = own_ref.shape
    shards = 2 * chips
    depth = shards * width
    rows = depth // PIECES
    core, is_first, chip_rank = flags[0], flags[1], flags[2]

    def in_copy(piece, which):
        span = pl.ds(piece * rows, rows)
        source = (wq, wk, wv)[which]
        return pltpu.make_async_copy(
            source.at[span, :],
            w_in.at[span, pl.ds(which * width, width)],
            sem_in.at[piece, which],
        )

    out_copy = pltpu.make_async_copy(wo, w_out, sem_out)
    for piece in range(PIECES):
        for which in range(3):
            in_copy(piece, which).start()
    out_copy.start()

    square = jnp.zeros((length, width), jnp.float32)
    for part in (own_ref, other_ref):
        for k in range(chips):
            value = part[k].astype(jnp.float32)
            square = square + value * value
    scale = lax.rsqrt(jnp.sum(square, axis=-1, keepdims=True) * (1.0 / depth) + EPSILON)
    for part, side in ((own_ref, core), (other_ref, 1 - core)):
        for k, (south, north) in enumerate(zip(*SHIFTS)):
            shift = jnp.where(side == 0, south, north)
            chip = lax.rem(chip_rank + chips - shift, chips)
            for h in range(2):
                shard = 2 * chip + (side if h == 0 else 1 - side)
                value = part[2 * k + h].astype(jnp.float32) * scale * gain_ref[shard]
                low = pl.multiple_of(shard * width, width)
                normed[:, pl.ds(low, width)] = value.astype(jnp.bfloat16)

    total = jnp.zeros((length, 3 * width), jnp.float32)
    for piece in range(PIECES):
        for which in range(3):
            in_copy(piece, which).wait()
        total = total + jnp.dot(
            normed[:, piece * rows : (piece + 1) * rows],
            w_in[piece * rows : (piece + 1) * rows, :],
            preferred_element_type=jnp.float32,
        )
    values = total[:, 2 * width :]
    source = jnp.where(is_first == 1, values.astype(jnp.bfloat16), source_ref[...])
    carried_ref[...] = source
    mix = mix_ref[...]
    mixed = (mix * values + (1.0 - mix) * source.astype(jnp.float32)).astype(jnp.bfloat16)
    cosine, sine = cos_ref[...], sin_ref[...]
    causal = lax.broadcasted_iota(jnp.int32, (length, length), 0) >= lax.broadcasted_iota(
        jnp.int32, (length, length), 1
    )

    def rotated(part):
        return (part * cosine + pltpu.roll(part, HEAD_DIM // 2, 1) * sine).astype(jnp.bfloat16)

    attended = []
    for head in range(width // HEAD_DIM):
        low = head * HEAD_DIM
        query = rotated(total[:, low : low + HEAD_DIM])
        key = rotated(total[:, width + low : width + low + HEAD_DIM])
        scores = lax.dot_general(
            query, key, (((1,), (1,)), ((), ())), preferred_element_type=jnp.float32
        ) * HEAD_DIM ** (-0.5)
        scores = jnp.where(causal, scores, -1e30)
        expo = jnp.exp(scores - jnp.max(scores, axis=-1, keepdims=True))
        probs = (expo / jnp.sum(expo, axis=-1, keepdims=True)).astype(jnp.bfloat16)
        attended.append(
            jnp.dot(
                probs, mixed[:, low : low + HEAD_DIM], preferred_element_type=jnp.float32
            ).astype(jnp.bfloat16)
        )
    attended = jnp.concatenate(attended, axis=-1)
    out_copy.wait()
    for chip in range(chips):
        for target, side in ((give_ref, 1 - core), (keep_ref, core)):
            low = pl.multiple_of((2 * chip + side) * width, width)
            target[chip] = jnp.dot(
                attended, w_out[:, pl.ds(low, width)], preferred_element_type=jnp.float32
            ).astype(jnp.bfloat16)


def run_layer(flags, own, other, gain, source, mix, cosine, sine, wq, wk, wv, wo):
    chips, length, width = own.shape
    depth = 2 * chips * width
    full = pl.BlockSpec(memory_space=VMEM)
    anywhere = pl.BlockSpec(memory_space=pl.ANY)
    half = jax.ShapeDtypeStruct((chips, length, width), jnp.bfloat16)
    return pl.pallas_call(
        layer_kernel,
        out_shape=(half, half, jax.ShapeDtypeStruct((length, width), jnp.bfloat16)),
        in_specs=[pl.BlockSpec(memory_space=pltpu.SMEM)] + [full] * 7 + [anywhere] * 4,
        out_specs=(full, full, full),
        scratch_shapes=[
            VMEM((length, depth), jnp.bfloat16),
            VMEM((depth, 3 * width), jnp.bfloat16),
            VMEM((width, depth), jnp.bfloat16),
            pltpu.SemaphoreType.DMA((PIECES, 3)),
            pltpu.SemaphoreType.DMA,
        ],
        compiler_params=pltpu.CompilerParams(vmem_limit_bytes=24 * 1024 * 1024),
        name="layer",
    )(flags, own, other, gain, source, mix, cosine, sine, wq, wk, wv, wo)


def close_kernel(flags, arrived_ref, own_ref, other_ref, old_ref, send_ref, outputs_ref):
    micro, core = flags[0], flags[1]
    here = 2 * SHIFTS[0].index(0)
    rows = jnp.where(core == 0, own_ref[here], other_ref[here + 1]).astype(jnp.float32)
    partial = arrived_ref[0].astype(jnp.float32)
    for j in range(1, arrived_ref.shape[0]):
        partial = partial + arrived_ref[j].astype(jnp.float32)
    fresh = (rows + partial).astype(jnp.bfloat16)
    send_ref[...] = fresh
    for m in range(outputs_ref.shape[0]):
        outputs_ref[m] = jnp.where(micro == m, fresh, old_ref[m])


def close_layer(flags, arrived, own, other, outputs):
    full = pl.BlockSpec(memory_space=VMEM)
    return pl.pallas_call(
        close_kernel,
        out_shape=(
            jax.ShapeDtypeStruct(own.shape[1:], jnp.bfloat16),
            jax.ShapeDtypeStruct(outputs.shape, jnp.bfloat16),
        ),
        in_specs=[pl.BlockSpec(memory_space=pltpu.SMEM)] + [full] * 4,
        out_specs=(full, full),
        compiler_params=pltpu.CompilerParams(vmem_limit_bytes=8 * 1024 * 1024),
        name="close",
    )(flags, arrived, own, other, outputs)


def shards(
    token_ids, emb_table, attn_gain, query_weight, key_weight, value_weight, mix_weight, out_weight
):
    section_rank = lax.axis_index("section")
    section_count = lax.axis_size("section")
    tensor_rank = lax.axis_index("tensor")
    tensor_count = lax.axis_size("tensor")
    batches, length = token_ids.shape
    vocab_local, width = emb_table.shape
    chips = tensor_count // 2
    same_core = [[2 * chip + core for chip in range(chips)] for core in range(2)]
    gain = attn_gain[0].astype(jnp.float32).reshape(tensor_count, 1, width)
    weights = (query_weight[0], key_weight[0], value_weight[0], out_weight[0])
    mix = jnp.repeat(mix_weight[0], HEAD_DIM)[None, :]
    cosine, sine = rotary_tables(length)
    is_first = (section_rank == 0).astype(jnp.int32)
    layer_flags = jnp.stack([lax.rem(tensor_rank, 2), is_first, tensor_rank // 2])
    layer_flags = layer_flags.astype(jnp.int32)

    flat_ids = token_ids.reshape(-1) - section_rank * vocab_local
    one_hot = (flat_ids[:, None] == jnp.arange(vocab_local, dtype=jnp.int32)[None, :]).astype(
        jnp.bfloat16
    )
    looked = jnp.dot(one_hot, emb_table, preferred_element_type=jnp.float32).astype(jnp.bfloat16)
    found = lax.all_to_all(
        jnp.broadcast_to(looked[None], (section_count, *looked.shape)), "section", 0, 0, tiled=True
    )
    first = found.astype(jnp.float32).sum(axis=0).astype(jnp.bfloat16)
    first = first.reshape(batches, length, width)
    partner = [(t, t ^ 1) for t in range(tensor_count)]
    both = ("section", "tensor")

    def ring(shifts):
        pairs = []
        for s in range(section_count):
            for t in range(tensor_count):
                target = (t + 2 * shifts[t % 2]) % tensor_count
                pairs.append((s * tensor_count + t, (s + 1) % section_count * tensor_count + target))
        return pairs

    first_pair = jnp.stack([first, lax.ppermute(first, "tensor", partner)], axis=1)

    def work(step, own, source, outputs):
        position = step - section_rank
        flags = jnp.stack([position, lax.rem(tensor_rank, 2)]).astype(jnp.int32)
        other = lax.ppermute(own, "tensor", partner)
        keep, give, carried = run_layer(
            layer_flags, own, other, gain, source, mix, cosine, sine, *weights
        )
        given = lax.ppermute(give, "tensor", partner)
        pair = (keep.astype(jnp.float32) + given.astype(jnp.float32)).astype(jnp.bfloat16)
        arrived = lax.all_to_all(pair, "tensor", 0, 0, axis_index_groups=same_core, tiled=True)
        send, outputs = close_layer(flags, arrived, own, other, outputs)
        send = jnp.stack([send, lax.ppermute(send, "tensor", partner)])
        return send, carried, outputs

    def rest(step, own, source, outputs):
        following = jnp.minimum(step + 1, batches - 1)
        send = lax.dynamic_index_in_dim(first_pair, following, 0, keepdims=False)
        return send, source, outputs

    def advance(step, state):
        send, carried, outputs = state
        own = jnp.concatenate(
            [lax.ppermute(send, both, ring(shifts)) for shifts in zip(*SHIFTS)]
        )
        source = lax.ppermute(carried, both, ring((0, 0)))
        position = step - section_rank
        active = (position >= 0) & (position < batches)
        return lax.cond(active, work, rest, step, own, source, outputs)

    carried = jnp.zeros((length, width), jnp.bfloat16)
    outputs = jnp.zeros((batches, length, width), jnp.bfloat16)
    step_count = batches + section_count - 1
    _, _, outputs = lax.fori_loop(0, step_count, advance, (first_pair[0], carried, outputs))
    return outputs[None]


def solution(mesh):
    in_specs = (
        P(),
        P("section", "tensor"),
        P("section", None),
        P("section", None, "tensor"),
        P("section", None, "tensor"),
        P("section", None, "tensor"),
        P("section", "tensor"),
        P("section", "tensor", None),
    )
    out_specs = P("section", None, None, "tensor")
    return jax.shard_map(shards, mesh=mesh, in_specs=in_specs, out_specs=out_specs, check_vma=False)
```

```python
import functools

import jax
import jax.numpy as jnp
from jax import lax
from jax.experimental import pallas as pl
from jax.experimental.pallas import tpu as pltpu
from jax.sharding import PartitionSpec as P

EPSILON = 1e-05
ROTARY_BASE = 10000.0
HEAD_DIM = 128
VMEM = pltpu.VMEM
PIECES = 4
SHIFTS = ((4, 1, 7, 0), (3, 5, 2, 6))
SPREAD = ((4, 3, 1, 0), (5, 2, 6, 7))


def rotary_tables(length):
    half_dim = HEAD_DIM // 2
    positions = jnp.arange(length, dtype=jnp.float32)
    frequency = ROTARY_BASE ** (-(jnp.arange(half_dim, dtype=jnp.float32) * 2.0) / HEAD_DIM)
    angles = positions[:, None] * frequency[None, :]
    cosine, sine = jnp.cos(angles), jnp.sin(angles)
    return (
        jnp.concatenate([cosine, cosine], axis=-1),
        jnp.concatenate([-sine, sine], axis=-1),
    )


def layer_kernel(
    flags, own_ref, other_ref, gain_ref, source_ref, mix_ref, cos_ref, sin_ref, wq, wk, wv, wo,
    keep_ref, give_ref, carried_ref, normed, w_in, w_out, sem_in, sem_out,
):
    chips, length, width = own_ref.shape
    shards = 2 * chips
    depth = shards * width
    rows = depth // PIECES
    core, is_first, chip_rank = flags[0], flags[1], flags[2]

    def in_copy(piece, which):
        span = pl.ds(piece * rows, rows)
        source = (wq, wk, wv)[which]
        return pltpu.make_async_copy(
            source.at[span, :],
            w_in.at[span, pl.ds(which * width, width)],
            sem_in.at[piece, which],
        )

    out_copy = pltpu.make_async_copy(wo, w_out, sem_out)
    for piece in range(PIECES):
        for which in range(3):
            in_copy(piece, which).start()
    out_copy.start()

    square = jnp.zeros((length, width), jnp.float32)
    for part in (own_ref, other_ref):
        for k in range(chips):
            value = part[k].astype(jnp.float32)
            square = square + value * value
    scale = lax.rsqrt(jnp.sum(square, axis=-1, keepdims=True) * (1.0 / depth) + EPSILON)
    for part, side in ((own_ref, core), (other_ref, 1 - core)):
        for k, (south, north) in enumerate(zip(*SHIFTS)):
            shift = jnp.where(side == 0, south, north)
            chip = lax.rem(chip_rank + chips - shift, chips)
            for h in range(2):
                shard = 2 * chip + h
                value = part[2 * k + h].astype(jnp.float32) * scale * gain_ref[shard]
                low = pl.multiple_of(shard * width, width)
                normed[:, pl.ds(low, width)] = value.astype(jnp.bfloat16)

    total = jnp.zeros((length, 3 * width), jnp.float32)
    for piece in range(PIECES):
        for which in range(3):
            in_copy(piece, which).wait()
        total = total + jnp.dot(
            normed[:, piece * rows : (piece + 1) * rows],
            w_in[piece * rows : (piece + 1) * rows, :],
            preferred_element_type=jnp.float32,
        )
    values = total[:, 2 * width :]
    source = jnp.where(is_first == 1, values.astype(jnp.bfloat16), source_ref[...])
    carried_ref[...] = source
    mix = mix_ref[...]
    mixed = (mix * values + (1.0 - mix) * source.astype(jnp.float32)).astype(jnp.bfloat16)
    cosine, sine = cos_ref[...], sin_ref[...]
    causal = lax.broadcasted_iota(jnp.int32, (length, length), 0) >= lax.broadcasted_iota(
        jnp.int32, (length, length), 1
    )

    def rotated(part):
        return (part * cosine + pltpu.roll(part, HEAD_DIM // 2, 1) * sine).astype(jnp.bfloat16)

    attended = []
    for head in range(width // HEAD_DIM):
        low = head * HEAD_DIM
        query = rotated(total[:, low : low + HEAD_DIM])
        key = rotated(total[:, width + low : width + low + HEAD_DIM])
        scores = lax.dot_general(
            query, key, (((1,), (1,)), ((), ())), preferred_element_type=jnp.float32
        ) * HEAD_DIM ** (-0.5)
        scores = jnp.where(causal, scores, -1e30)
        expo = jnp.exp(scores - jnp.max(scores, axis=-1, keepdims=True))
        probs = (expo / jnp.sum(expo, axis=-1, keepdims=True)).astype(jnp.bfloat16)
        attended.append(
            jnp.dot(
                probs, mixed[:, low : low + HEAD_DIM], preferred_element_type=jnp.float32
            ).astype(jnp.bfloat16)
        )
    attended = jnp.concatenate(attended, axis=-1)
    out_copy.wait()
    for target, side in ((give_ref, 1 - core), (keep_ref, core)):
        for k, (south, north) in enumerate(zip(*SPREAD)):
            shift = jnp.where(side == 0, south, north)
            chip = lax.rem(chip_rank + shift, chips)
            for h in range(2):
                low = pl.multiple_of((2 * chip + h) * width, width)
                target[2 * k + h] = jnp.dot(
                    attended, w_out[:, pl.ds(low, width)], preferred_element_type=jnp.float32
                ).astype(jnp.bfloat16)


def run_layer(flags, own, other, gain, source, mix, cosine, sine, wq, wk, wv, wo):
    chips, length, width = own.shape
    depth = 2 * chips * width
    full = pl.BlockSpec(memory_space=VMEM)
    anywhere = pl.BlockSpec(memory_space=pl.ANY)
    half = jax.ShapeDtypeStruct((chips, length, width), jnp.bfloat16)
    return pl.pallas_call(
        layer_kernel,
        out_shape=(half, half, jax.ShapeDtypeStruct((length, width), jnp.bfloat16)),
        in_specs=[pl.BlockSpec(memory_space=pltpu.SMEM)] + [full] * 7 + [anywhere] * 4,
        out_specs=(full, full, full),
        scratch_shapes=[
            VMEM((length, depth), jnp.bfloat16),
            VMEM((depth, 3 * width), jnp.bfloat16),
            VMEM((width, depth), jnp.bfloat16),
            pltpu.SemaphoreType.DMA((PIECES, 3)),
            pltpu.SemaphoreType.DMA,
        ],
        compiler_params=pltpu.CompilerParams(vmem_limit_bytes=24 * 1024 * 1024),
        name="layer",
    )(flags, own, other, gain, source, mix, cosine, sine, wq, wk, wv, wo)


def pair_kernel(keep_ref, given_ref, *out_refs):
    for k, out_ref in enumerate(out_refs):
        for h in range(2):
            kept = keep_ref[2 * k + h].astype(jnp.float32)
            out_ref[h] = (kept + given_ref[2 * k + h].astype(jnp.float32)).astype(jnp.bfloat16)


def pair_up(keep, given):
    full = pl.BlockSpec(memory_space=VMEM)
    count = keep.shape[0] // 2
    shape = jax.ShapeDtypeStruct((2, *keep.shape[1:]), jnp.bfloat16)
    return pl.pallas_call(
        pair_kernel,
        out_shape=(shape,) * count,
        in_specs=[full] * 2,
        out_specs=(full,) * count,
        compiler_params=pltpu.CompilerParams(vmem_limit_bytes=4 * 1024 * 1024),
        name="pair",
    )(keep, given)


def gather_kernel(*refs):
    out_ref = refs[-1]
    for h in range(2):
        total = refs[0][h].astype(jnp.float32)
        for ref in refs[1:-1]:
            total = total + ref[h].astype(jnp.float32)
        out_ref[h] = total.astype(jnp.bfloat16)


def gather_up(pieces):
    full = pl.BlockSpec(memory_space=VMEM)
    return pl.pallas_call(
        gather_kernel,
        out_shape=jax.ShapeDtypeStruct(pieces[0].shape, jnp.bfloat16),
        in_specs=[full] * len(pieces),
        out_specs=full,
        compiler_params=pltpu.CompilerParams(vmem_limit_bytes=4 * 1024 * 1024),
        name="gather",
    )(*pieces)


def close_kernel(flags, mine_ref, theirs_ref, own_ref, other_ref, old_ref, send_ref, outputs_ref):
    micro, core = flags[0], flags[1]
    here = 2 * SHIFTS[0].index(0)
    fresh = []
    for h in range(2):
        rows = jnp.where(core == 0, own_ref[here + h], other_ref[here + h]).astype(jnp.float32)
        partial = mine_ref[h].astype(jnp.float32) + theirs_ref[h].astype(jnp.float32)
        fresh.append((rows + partial).astype(jnp.bfloat16))
        send_ref[h] = fresh[h]
    local = jnp.where(core == 0, fresh[0], fresh[1])
    for m in range(outputs_ref.shape[0]):
        outputs_ref[m] = jnp.where(micro == m, local, old_ref[m])


def close_layer(flags, mine, theirs, own, other, outputs):
    full = pl.BlockSpec(memory_space=VMEM)
    return pl.pallas_call(
        close_kernel,
        out_shape=(
            jax.ShapeDtypeStruct(mine.shape, jnp.bfloat16),
            jax.ShapeDtypeStruct(outputs.shape, jnp.bfloat16),
        ),
        in_specs=[pl.BlockSpec(memory_space=pltpu.SMEM)] + [full] * 5,
        out_specs=(full, full),
        compiler_params=pltpu.CompilerParams(vmem_limit_bytes=8 * 1024 * 1024),
        name="close",
    )(flags, mine, theirs, own, other, outputs)


def shards(
    token_ids, emb_table, attn_gain, query_weight, key_weight, value_weight, mix_weight, out_weight
):
    section_rank = lax.axis_index("section")
    section_count = lax.axis_size("section")
    tensor_rank = lax.axis_index("tensor")
    tensor_count = lax.axis_size("tensor")
    batches, length = token_ids.shape
    vocab_local, width = emb_table.shape
    chips = tensor_count // 2
    gain = attn_gain[0].astype(jnp.float32).reshape(tensor_count, 1, width)
    weights = (query_weight[0], key_weight[0], value_weight[0], out_weight[0])
    mix = jnp.repeat(mix_weight[0], HEAD_DIM)[None, :]
    cosine, sine = rotary_tables(length)
    is_first = (section_rank == 0).astype(jnp.int32)
    layer_flags = jnp.stack([lax.rem(tensor_rank, 2), is_first, tensor_rank // 2])
    layer_flags = layer_flags.astype(jnp.int32)

    flat_ids = token_ids.reshape(-1) - section_rank * vocab_local
    one_hot = (flat_ids[:, None] == jnp.arange(vocab_local, dtype=jnp.int32)[None, :]).astype(
        jnp.bfloat16
    )
    looked = jnp.dot(one_hot, emb_table, preferred_element_type=jnp.float32).astype(jnp.bfloat16)
    found = lax.all_to_all(
        jnp.broadcast_to(looked[None], (section_count, *looked.shape)), "section", 0, 0, tiled=True
    )
    first = found.astype(jnp.float32).sum(axis=0).astype(jnp.bfloat16)
    first = first.reshape(batches, length, width)
    partner = [(t, t ^ 1) for t in range(tensor_count)]
    both = ("section", "tensor")

    def ring(shifts):
        pairs = []
        for s in range(section_count):
            for t in range(tensor_count):
                target = (t + 2 * shifts[t % 2]) % tensor_count
                pairs.append((s * tensor_count + t, (s + 1) % section_count * tensor_count + target))
        return pairs

    def spread(shifts):
        return [(t, (t + 2 * shifts[t % 2]) % tensor_count) for t in range(tensor_count)]

    swapped = lax.ppermute(first, "tensor", partner)
    is_south = lax.rem(tensor_rank, 2) == 0
    first_pair = jnp.stack(
        [jnp.where(is_south, first, swapped), jnp.where(is_south, swapped, first)], axis=1
    )

    def work(step, own, source, outputs):
        position = step - section_rank
        flags = jnp.stack([position, lax.rem(tensor_rank, 2)]).astype(jnp.int32)
        other = lax.ppermute(own, "tensor", partner)
        keep, give, carried = run_layer(
            layer_flags, own, other, gain, source, mix, cosine, sine, *weights
        )
        given = lax.ppermute(give, "tensor", partner)
        pairs = pair_up(keep, given)
        mine = gather_up(
            [
                lax.ppermute(piece, "tensor", spread(shifts))
                for piece, shifts in zip(pairs, zip(*SPREAD))
            ]
        )
        theirs = lax.ppermute(mine, "tensor", partner)
        send, outputs = close_layer(flags, mine, theirs, own, other, outputs)
        return send, carried, outputs

    def rest(step, own, source, outputs):
        following = jnp.minimum(step + 1, batches - 1)
        send = lax.dynamic_index_in_dim(first_pair, following, 0, keepdims=False)
        return send, source, outputs

    def advance(step, state):
        send, carried, outputs = state
        own = jnp.concatenate(
            [lax.ppermute(send, both, ring(shifts)) for shifts in zip(*SHIFTS)]
        )
        source = lax.ppermute(carried, both, ring((0, 0)))
        position = step - section_rank
        active = (position >= 0) & (position < batches)
        return lax.cond(active, work, rest, step, own, source, outputs)

    carried = jnp.zeros((length, width), jnp.bfloat16)
    outputs = jnp.zeros((batches, length, width), jnp.bfloat16)
    step_count = batches + section_count - 1
    _, _, outputs = lax.fori_loop(0, step_count, advance, (first_pair[0], carried, outputs))
    return outputs[None]


def solution(mesh):
    in_specs = (
        P(),
        P("section", "tensor"),
        P("section", None),
        P("section", None, "tensor"),
        P("section", None, "tensor"),
        P("section", None, "tensor"),
        P("section", "tensor"),
        P("section", "tensor", None),
    )
    out_specs = P("section", None, None, "tensor")
    return jax.shard_map(shards, mesh=mesh, in_specs=in_specs, out_specs=out_specs, check_vma=False)
```

```python
import functools

import jax
import jax.numpy as jnp
from jax import lax
from jax.experimental import pallas as pl
from jax.experimental.pallas import tpu as pltpu
from jax.sharding import PartitionSpec as P

EPSILON = 1e-05
ROTARY_BASE = 10000.0
HEAD_DIM = 128
VMEM = pltpu.VMEM
PIECES = 4
SHIFTS = ((0, 7, 2, 4), (1, 6, 3, 5))
SPREAD = ((4, 3, 1, 0), (5, 2, 6, 7))


def rotary_tables(length):
    half_dim = HEAD_DIM // 2
    positions = jnp.arange(length, dtype=jnp.float32)
    frequency = ROTARY_BASE ** (-(jnp.arange(half_dim, dtype=jnp.float32) * 2.0) / HEAD_DIM)
    angles = positions[:, None] * frequency[None, :]
    cosine, sine = jnp.cos(angles), jnp.sin(angles)
    return (
        jnp.concatenate([cosine, cosine], axis=-1),
        jnp.concatenate([-sine, sine], axis=-1),
    )


def layer_kernel(
    flags, own_ref, other_ref, gain_ref, source_ref, mix_ref, cos_ref, sin_ref, wq, wk, wv, wo,
    keep_ref, give_ref, carried_ref, normed, w_in, w_out, sem_in, sem_out,
):
    chips, length, width = own_ref.shape
    shards = 2 * chips
    depth = shards * width
    rows = depth // PIECES
    core, is_first, chip_rank = flags[0], flags[1], flags[2]

    def in_copy(piece, which):
        span = pl.ds(piece * rows, rows)
        source = (wq, wk, wv)[which]
        return pltpu.make_async_copy(
            source.at[span, :],
            w_in.at[span, pl.ds(which * width, width)],
            sem_in.at[piece, which],
        )

    out_copy = pltpu.make_async_copy(wo, w_out, sem_out)
    for piece in range(PIECES):
        for which in range(3):
            in_copy(piece, which).start()
    out_copy.start()

    square = jnp.zeros((length, width), jnp.float32)
    for part in (own_ref, other_ref):
        for k in range(chips):
            value = part[k].astype(jnp.float32)
            square = square + value * value
    scale = lax.rsqrt(jnp.sum(square, axis=-1, keepdims=True) * (1.0 / depth) + EPSILON)
    for part, side in ((own_ref, core), (other_ref, 1 - core)):
        for k, (south, north) in enumerate(zip(*SHIFTS)):
            shift = jnp.where(side == 0, south, north)
            chip = lax.rem(chip_rank + chips - shift, chips)
            for h in range(2):
                shard = 2 * chip + h
                value = part[2 * k + h].astype(jnp.float32) * scale * gain_ref[shard]
                low = pl.multiple_of(shard * width, width)
                normed[:, pl.ds(low, width)] = value.astype(jnp.bfloat16)

    total = jnp.zeros((length, 3 * width), jnp.float32)
    for piece in range(PIECES):
        for which in range(3):
            in_copy(piece, which).wait()
        total = total + jnp.dot(
            normed[:, piece * rows : (piece + 1) * rows],
            w_in[piece * rows : (piece + 1) * rows, :],
            preferred_element_type=jnp.float32,
        )
    values = total[:, 2 * width :]
    source = jnp.where(is_first == 1, values.astype(jnp.bfloat16), source_ref[...])
    carried_ref[...] = source
    mix = mix_ref[...]
    mixed = (mix * values + (1.0 - mix) * source.astype(jnp.float32)).astype(jnp.bfloat16)
    cosine, sine = cos_ref[...], sin_ref[...]
    causal = lax.broadcasted_iota(jnp.int32, (length, length), 0) >= lax.broadcasted_iota(
        jnp.int32, (length, length), 1
    )

    def rotated(part):
        return (part * cosine + pltpu.roll(part, HEAD_DIM // 2, 1) * sine).astype(jnp.bfloat16)

    attended = []
    for head in range(width // HEAD_DIM):
        low = head * HEAD_DIM
        query = rotated(total[:, low : low + HEAD_DIM])
        key = rotated(total[:, width + low : width + low + HEAD_DIM])
        scores = lax.dot_general(
            query, key, (((1,), (1,)), ((), ())), preferred_element_type=jnp.float32
        ) * HEAD_DIM ** (-0.5)
        scores = jnp.where(causal, scores, -1e30)
        expo = jnp.exp(scores - jnp.max(scores, axis=-1, keepdims=True))
        probs = (expo / jnp.sum(expo, axis=-1, keepdims=True)).astype(jnp.bfloat16)
        attended.append(
            jnp.dot(
                probs, mixed[:, low : low + HEAD_DIM], preferred_element_type=jnp.float32
            ).astype(jnp.bfloat16)
        )
    attended = jnp.concatenate(attended, axis=-1)
    out_copy.wait()
    for target, side in ((give_ref, 1 - core), (keep_ref, core)):
        for k, (south, north) in enumerate(zip(*SPREAD)):
            shift = jnp.where(side == 0, south, north)
            chip = lax.rem(chip_rank + shift, chips)
            for h in range(2):
                low = pl.multiple_of((2 * chip + h) * width, width)
                target[2 * k + h] = jnp.dot(
                    attended, w_out[:, pl.ds(low, width)], preferred_element_type=jnp.float32
                ).astype(jnp.bfloat16)


def run_layer(flags, own, other, gain, source, mix, cosine, sine, wq, wk, wv, wo):
    chips, length, width = own.shape
    depth = 2 * chips * width
    full = pl.BlockSpec(memory_space=VMEM)
    anywhere = pl.BlockSpec(memory_space=pl.ANY)
    half = jax.ShapeDtypeStruct((chips, length, width), jnp.bfloat16)
    return pl.pallas_call(
        layer_kernel,
        out_shape=(half, half, jax.ShapeDtypeStruct((length, width), jnp.bfloat16)),
        in_specs=[pl.BlockSpec(memory_space=pltpu.SMEM)] + [full] * 7 + [anywhere] * 4,
        out_specs=(full, full, full),
        scratch_shapes=[
            VMEM((length, depth), jnp.bfloat16),
            VMEM((depth, 3 * width), jnp.bfloat16),
            VMEM((width, depth), jnp.bfloat16),
            pltpu.SemaphoreType.DMA((PIECES, 3)),
            pltpu.SemaphoreType.DMA,
        ],
        compiler_params=pltpu.CompilerParams(vmem_limit_bytes=24 * 1024 * 1024),
        name="layer",
    )(flags, own, other, gain, source, mix, cosine, sine, wq, wk, wv, wo)


def pair_kernel(keep_ref, given_ref, *out_refs):
    for k, out_ref in enumerate(out_refs):
        for h in range(2):
            kept = keep_ref[2 * k + h].astype(jnp.float32)
            out_ref[h] = (kept + given_ref[2 * k + h].astype(jnp.float32)).astype(jnp.bfloat16)


def pair_up(keep, given):
    full = pl.BlockSpec(memory_space=VMEM)
    count = keep.shape[0] // 2
    shape = jax.ShapeDtypeStruct((2, *keep.shape[1:]), jnp.bfloat16)
    return pl.pallas_call(
        pair_kernel,
        out_shape=(shape,) * count,
        in_specs=[full] * 2,
        out_specs=(full,) * count,
        compiler_params=pltpu.CompilerParams(vmem_limit_bytes=4 * 1024 * 1024),
        name="pair",
    )(keep, given)


def gather_kernel(*refs):
    out_ref = refs[-1]
    for h in range(2):
        total = refs[0][h].astype(jnp.float32)
        for ref in refs[1:-1]:
            total = total + ref[h].astype(jnp.float32)
        out_ref[h] = total.astype(jnp.bfloat16)


def gather_up(pieces):
    full = pl.BlockSpec(memory_space=VMEM)
    return pl.pallas_call(
        gather_kernel,
        out_shape=jax.ShapeDtypeStruct(pieces[0].shape, jnp.bfloat16),
        in_specs=[full] * len(pieces),
        out_specs=full,
        compiler_params=pltpu.CompilerParams(vmem_limit_bytes=4 * 1024 * 1024),
        name="gather",
    )(*pieces)


def close_kernel(flags, mine_ref, theirs_ref, own_ref, other_ref, old_ref, send_ref, outputs_ref):
    micro, core = flags[0], flags[1]
    here = 2 * SHIFTS[0].index(0)
    fresh = []
    for h in range(2):
        rows = jnp.where(core == 0, own_ref[here + h], other_ref[here + h]).astype(jnp.float32)
        partial = mine_ref[h].astype(jnp.float32) + theirs_ref[h].astype(jnp.float32)
        fresh.append((rows + partial).astype(jnp.bfloat16))
        send_ref[h] = fresh[h]
    local = jnp.where(core == 0, fresh[0], fresh[1])
    for m in range(outputs_ref.shape[0]):
        outputs_ref[m] = jnp.where(micro == m, local, old_ref[m])


def close_layer(flags, mine, theirs, own, other, outputs):
    full = pl.BlockSpec(memory_space=VMEM)
    return pl.pallas_call(
        close_kernel,
        out_shape=(
            jax.ShapeDtypeStruct(mine.shape, jnp.bfloat16),
            jax.ShapeDtypeStruct(outputs.shape, jnp.bfloat16),
        ),
        in_specs=[pl.BlockSpec(memory_space=pltpu.SMEM)] + [full] * 5,
        out_specs=(full, full),
        compiler_params=pltpu.CompilerParams(vmem_limit_bytes=8 * 1024 * 1024),
        name="close",
    )(flags, mine, theirs, own, other, outputs)


def shards(
    token_ids, emb_table, attn_gain, query_weight, key_weight, value_weight, mix_weight, out_weight
):
    section_rank = lax.axis_index("section")
    section_count = lax.axis_size("section")
    tensor_rank = lax.axis_index("tensor")
    tensor_count = lax.axis_size("tensor")
    batches, length = token_ids.shape
    vocab_local, width = emb_table.shape
    chips = tensor_count // 2
    gain = attn_gain[0].astype(jnp.float32).reshape(tensor_count, 1, width)
    weights = (query_weight[0], key_weight[0], value_weight[0], out_weight[0])
    mix = jnp.repeat(mix_weight[0], HEAD_DIM)[None, :]
    cosine, sine = rotary_tables(length)
    is_first = (section_rank == 0).astype(jnp.int32)
    layer_flags = jnp.stack([lax.rem(tensor_rank, 2), is_first, tensor_rank // 2])
    layer_flags = layer_flags.astype(jnp.int32)

    flat_ids = token_ids.reshape(-1) - section_rank * vocab_local
    one_hot = (flat_ids[:, None] == jnp.arange(vocab_local, dtype=jnp.int32)[None, :]).astype(
        jnp.bfloat16
    )
    looked = jnp.dot(one_hot, emb_table, preferred_element_type=jnp.float32).astype(jnp.bfloat16)
    found = lax.all_to_all(
        jnp.broadcast_to(looked[None], (section_count, *looked.shape)), "section", 0, 0, tiled=True
    )
    first = found.astype(jnp.float32).sum(axis=0).astype(jnp.bfloat16)
    first = first.reshape(batches, length, width)
    partner = [(t, t ^ 1) for t in range(tensor_count)]
    both = ("section", "tensor")

    def ring(shifts):
        pairs = []
        for s in range(section_count):
            for t in range(tensor_count):
                target = (t + 2 * shifts[t % 2]) % tensor_count
                pairs.append((s * tensor_count + t, (s + 1) % section_count * tensor_count + target))
        return pairs

    def spread(shifts):
        return [(t, (t + 2 * shifts[t % 2]) % tensor_count) for t in range(tensor_count)]

    swapped = lax.ppermute(first, "tensor", partner)
    is_south = lax.rem(tensor_rank, 2) == 0
    first_pair = jnp.stack(
        [jnp.where(is_south, first, swapped), jnp.where(is_south, swapped, first)], axis=1
    )

    def work(step, own, source, outputs):
        position = step - section_rank
        flags = jnp.stack([position, lax.rem(tensor_rank, 2)]).astype(jnp.int32)
        other = lax.ppermute(own, "tensor", partner)
        keep, give, carried = run_layer(
            layer_flags, own, other, gain, source, mix, cosine, sine, *weights
        )
        given = lax.ppermute(give, "tensor", partner)
        pairs = pair_up(keep, given)
        mine = gather_up(
            [
                lax.ppermute(piece, "tensor", spread(shifts))
                for piece, shifts in zip(pairs, zip(*SPREAD))
            ]
        )
        theirs = lax.ppermute(mine, "tensor", partner)
        send, outputs = close_layer(flags, mine, theirs, own, other, outputs)
        return send, carried, outputs

    def rest(step, own, source, outputs):
        following = jnp.minimum(step + 1, batches - 1)
        send = lax.dynamic_index_in_dim(first_pair, following, 0, keepdims=False)
        return send, source, outputs

    def advance(step, state):
        send, carried, outputs = state
        own = jnp.concatenate(
            [lax.ppermute(send, both, ring(shifts)) for shifts in zip(*SHIFTS)]
        )
        source = lax.ppermute(carried, both, ring((0, 0)))
        position = step - section_rank
        active = (position >= 0) & (position < batches)
        return lax.cond(active, work, rest, step, own, source, outputs)

    carried = jnp.zeros((length, width), jnp.bfloat16)
    outputs = jnp.zeros((batches, length, width), jnp.bfloat16)
    step_count = batches + section_count - 1
    _, _, outputs = lax.fori_loop(0, step_count, advance, (first_pair[0], carried, outputs))
    return outputs[None]


def solution(mesh):
    in_specs = (
        P(),
        P("section", "tensor"),
        P("section", None),
        P("section", None, "tensor"),
        P("section", None, "tensor"),
        P("section", None, "tensor"),
        P("section", "tensor"),
        P("section", "tensor", None),
    )
    out_specs = P("section", None, None, "tensor")
    return jax.shard_map(shards, mesh=mesh, in_specs=in_specs, out_specs=out_specs, check_vma=False)
```
